32 devices in a mesh: tile: 2 (over y), beam: 4 (over z), bl: 2 (over x), pol: 2 (over core).
Axes of the slice: x: 2, y: 2, z: 4, core: 2. Of those that a mesh axis runs over, the one named last changes fastest.
Arguments:
- sky_model: bfloat16 [4096, 4096], P(('tile', 'bl', 'pol'), 'beam'), parts along dimension 0, may hold values from -6 to 6
- beam_pattern: bfloat16 [8, 2048, 2048], P(('tile', 'beam'), ('bl', 'pol')), parts along dimension 0, may hold values from 0.099609375 to 1
- kernels: bfloat16 [8, 256, 128, 128], P(('tile', 'beam'), ('bl', 'pol')), parts along dimension 0, may hold values from -0.5 to 0.5
- observed: float32 [8, 256, 2, 128], P(('tile', 'beam'), ('bl', 'pol')), parts along dimension 0, may hold values from -6 to 6
- tile_owner: int32 [8, 256, 1], P(('tile', 'beam'), ('bl', 'pol')), parts along dimension 0, may hold values from 0 to 3; in each aligned block of 64 rows (0 to 63, 64 to 127, ..., all dimensions but the last counted through in order) at most 32 rows name the same one
- tile_local: int32 [8, 256], P(('tile', 'beam'), ('bl', 'pol')), parts along dimension 0, may hold values from 0 to 4095
- vis_count: int32 [8, 256], P(('tile', 'beam'), ('bl', 'pol')), parts along dimension 0, may hold values from 1 to 128
Outputs:
- residual_vis: float32 [8, 256, 2, 128], P(('tile', 'beam'), ('bl', 'pol')), parts along dimension 0
- dirty_grid: float32 [8, 16384, 2, 128], P(('tile', 'beam'), ('bl', 'pol')), parts along dimension 0
The draws below stay inside these ranges and needn't reach their ends.
There are 2 independent parts, one for each index of `tile`. The reference program is written for one: setup_inputs(seed, part) draws one part's arguments, and reference() takes and returns one part's arrays. A program takes and returns all parts, laid end to end along the dimension named above; each array names one. Nothing has to cross between parts.
Inputs may be any that keep to these rules, and one draw needn't show every extreme that they name: `tile_owner`: among the 64 visibility tiles of one device, at most 32 name the same owner, and in some blocks one owner is named exactly 32 times.
All inputs are finite; a program needn't handle non-finite values.
Results may differ from the reference program's by a relative error of at most 0.0055.
Values may be sent and summed in bfloat16 or wider, within the bound.
A program may use at most 64 MiB of HBM per device.

```python
import math
import jax
import jax.numpy as jnp
import numpy as np
from jax import lax

GRID = 2048
TILE_VIS = 128
VIS_DEV = 64
BEAMS = 4
GROUP = 4
STRIDE = 1024
HALO = 512
SKY_COLS = 4096
TILES_DEV = 4096
TILES_ALL = 16384
VIS_ALL = 256
CAP = 32


def set_ends(values, own_key, smallest, top_value):
    extent = values.shape
    index_at = [jax.random.randint(jax.random.fold_in(own_key, axis), (), 0, extent[axis]) for axis in range(len(extent))]
    values = values.at[tuple(index_at)].set(smallest)
    longest = extent.index(max(extent))
    index_at[longest] = (index_at[longest] + 1) % extent[longest]
    return values.at[tuple(index_at)].set(top_value)


def steps_of(stream_key, extent, shards, smallest, high):
    factor_of = 1.0
    for position, parts in shards:
        heights = jax.random.uniform(jax.random.fold_in(jax.random.fold_in(stream_key, 6), position), (parts,), jnp.float32, smallest / len(shards), high / len(shards))
        factor_of = factor_of * jnp.repeat(jnp.exp(heights), extent[position] // parts).reshape((-1,) + (1,) * (len(extent) - 1 - position))
    return factor_of


def shared_out(stream_key, own, number, rows, number_of, top, limit, skew):
    sequence = jax.random.permutation(stream_key, number_of)
    heavy_load, ordinary = shares(number_of, rows * top, limit, skew, True), shares(number_of, rows * top, limit, skew, False)
    places = jnp.arange(number_of)

    def named(tallies, rotation):
        used = int((tallies > 0).sum())
        fixed = max(1, used // 4)
        passed = fixed + (places - fixed + rotation * (used - fixed)) % max(1, number_of - fixed)
        return jnp.zeros((number_of,), jnp.int32).at[sequence[jnp.where(places < fixed, places, passed)]].set(jnp.asarray(tallies, jnp.int32))

    tallies = jnp.where(number % 4 == 0, named(heavy_load, number // 4), named(ordinary, number - number // 4 - 1))
    mixed = jax.random.permutation(jax.random.fold_in(own, 3), number_of)
    donor, taker = mixed[0:number_of // 2 * 2:2], mixed[1:number_of // 2 * 2:2]
    room = jnp.minimum(tallies[donor] - 1, limit - tallies[taker]) // 2
    room = jnp.where((donor == sequence[0]) | (taker == sequence[0]) | (tallies[taker] == 0), 0, jnp.maximum(room, 0))
    passed = jax.random.randint(jax.random.fold_in(own, 4), (number_of // 2,), 0, 1 << 20) % (room + 1)
    tallies = tallies.at[donor].add(-passed).at[taker].add(passed)
    items = jnp.searchsorted(jnp.cumsum(tallies), jnp.arange(rows * top), side="right").astype(jnp.int32)
    listing = items.reshape(top, rows).T
    listing = listing[jax.random.permutation(jax.random.fold_in(own, 1), rows)]
    rotation = jax.random.randint(jax.random.fold_in(own, 2), (rows, 1), 0, top)
    return jnp.take_along_axis(listing, (jnp.arange(top)[None, :] + rotation) % top, axis=1)


def shares(count, total, limit, slope, full):
    weights = [(1 << 20) // math.isqrt(rank ** slope) + 1 for rank in range(1, count + 1)]
    largest = limit if full else min(limit, max(-(-total // count), total * weights[0] // sum(weights)))
    least = 1 if total - largest >= count - 1 else 0
    given, spare = [largest] + [least] * (count - 1), total - largest - least * (count - 1)
    while spare > 0:
        free = [i for i in range(1, count) if given[i] < largest] or [i for i in range(1, count) if given[i] < limit]
        pool, left = sum([weights[i] for i in free]), spare
        for i in free:
            extra = min(limit - given[i], max(1, left * weights[i] // pool), spare)
            given[i] = given[i] + extra
            spare = spare - extra
    return np.array(given)


def scatter_about(key, dims, spread, most, split=(), held_as=jnp.bfloat16):
    array = spread * jax.random.normal(key, dims, jnp.float32)
    if split:
        array = array * steps_of(key, dims, split, -0.22, 0.18)
    return jnp.clip(array, -most, most).astype(held_as)


def setup_inputs(seed: int = 0, part: int = 0) -> dict:
    arg_keys = jax.random.split(jax.random.key(seed), 8)
    part_keys = jax.random.split(jax.random.fold_in(arg_keys[7], part), 8)
    sky_model = scatter_about(part_keys[0], (GRID, SKY_COLS), 1.0, 6.0, ((0, 4), (1, 4)))
    beam_pattern = jnp.clip(0.099609375 + 0.9003906 * jax.random.uniform(part_keys[1], (BEAMS, GRID, GRID), jnp.float32) ** steps_of(part_keys[1], (BEAMS, GRID, GRID), ((0, 4), (1, 4)), -0.2, 0.2), 0.099609375, 1.0).astype(jnp.bfloat16)
    kernels = scatter_about(part_keys[2], (BEAMS, VIS_ALL, TILE_VIS, TILE_VIS), TILE_VIS ** -0.5, 0.5, ((0, 4), (1, 4)))
    observed = scatter_about(part_keys[3], (BEAMS, VIS_ALL, 2, TILE_VIS), 1.0, 6.0, ((0, 4), (1, 4)), jnp.float32)
    tile_owner_keys = jax.random.split(jax.random.fold_in(part_keys[4], 1), BEAMS * VIS_ALL // VIS_DEV)
    tile_owner_turns = jax.random.permutation(jax.random.fold_in(part_keys[4], 3), BEAMS * VIS_ALL // VIS_DEV)
    tile_owner = jax.vmap(lambda own, number: shared_out(jax.random.fold_in(part_keys[4], 2), own, number, VIS_DEV, GROUP, 1, CAP, 2))(tile_owner_keys, tile_owner_turns).reshape((BEAMS, VIS_ALL, 1))
    tile_local = set_ends(jax.random.randint(part_keys[5], (BEAMS, VIS_ALL), 0, TILES_DEV), jax.random.fold_in(part_keys[5], 1), 0, TILES_DEV - 1).astype(jnp.int32)
    vis_count = set_ends(jax.random.randint(part_keys[6], (BEAMS, VIS_ALL), 1, TILE_VIS + 1), jax.random.fold_in(part_keys[6], 1), 1, TILE_VIS).astype(jnp.int32)
    return {"sky_model": sky_model, "beam_pattern": beam_pattern, "kernels": kernels, "observed": observed, "tile_owner": tile_owner, "tile_local": tile_local, "vis_count": vis_count}


def tables(rows, cols):
    row_index = jnp.arange(rows, dtype=jnp.int32)[:, None]
    col_index = jnp.arange(cols, dtype=jnp.int32)[None, :]
    angles = (row_index * col_index % GRID).astype(jnp.float32) * jnp.float32(2.0 * math.pi / GRID)
    factor = jnp.float32(1.0 / math.sqrt(GRID))
    return ((jnp.cos(angles) * factor).astype(jnp.bfloat16), (jnp.sin(angles) * factor).astype(jnp.bfloat16))

def product(left, right):
    return jnp.dot(left.astype(jnp.float32), right.astype(jnp.float32), precision=lax.Precision.HIGHEST)

def reference(sky_model, beam_pattern, kernels, observed, tile_owner, tile_local, vis_count):
    cos_one, sin_one = tables(GRID // 2, GRID)
    cos_two, sin_two = tables(GRID, GRID)
    padded = jnp.pad(sky_model, ((0, 0), (HALO, HALO)))

    def one_beam(packed):
        beam_no, pattern, kernel_set, seen, owners, local_ids, counts = packed
        window = lax.dynamic_slice_in_dim(padded, (beam_no * STRIDE).astype(jnp.int32), GRID, 1)
        apparent = (pattern.astype(jnp.float32) * window.astype(jnp.float32)).astype(jnp.bfloat16)
        half_real = product(cos_one, apparent.T).astype(jnp.bfloat16)
        half_imag = (-product(sin_one, apparent.T)).astype(jnp.bfloat16)
        uv_real = product(half_real, cos_two) + product(half_imag, sin_two)
        uv_imag = product(half_imag, cos_two) - product(half_real, sin_two)
        uv_grid = jnp.stack([uv_real, uv_imag]).astype(jnp.bfloat16)
        uv_tiles = uv_grid.reshape(2, GRID // 16, 8, GRID // 16, 16).transpose(1, 3, 0, 2, 4).reshape(TILES_ALL, 2, TILE_VIS)
        tile_index = (owners * TILES_DEV + local_ids).astype(jnp.int32)
        fetched = uv_tiles[tile_index]
        kernel_wide = kernel_set.astype(jnp.float32)
        predicted = jnp.einsum('rjm,rcm->rcj', kernel_wide, fetched.astype(jnp.float32), precision=lax.Precision.HIGHEST)
        live_mask = jnp.arange(TILE_VIS, dtype=jnp.int32)[None, :] < counts[:, None]
        residual = jnp.where(live_mask[:, None, :], seen - predicted, jnp.zeros_like(predicted))
        residual_low = residual.astype(jnp.bfloat16)
        contribution = jnp.einsum('rjm,rcj->rcm', kernel_wide, residual_low.astype(jnp.float32), precision=lax.Precision.HIGHEST)
        dirty = jax.ops.segment_sum(contribution, tile_index, num_segments=TILES_ALL)
        return (residual, dirty)
    beam_numbers = jnp.arange(BEAMS, dtype=jnp.int32)
    residual_vis, dirty_grid = lax.map(one_beam, (beam_numbers, beam_pattern, kernels, observed, tile_owner[:, :, 0], tile_local, vis_count))
    return (residual_vis, dirty_grid)
```

```python
import functools
import math

import jax
import jax.numpy as jnp
import numpy as np
from jax import lax
from jax.experimental import pallas as pl
from jax.experimental.pallas import tpu as pltpu
from jax.sharding import PartitionSpec as P

MESH = pl.DeviceIdType.MESH
RADIX = 8
WIDE = 16
VMEM = pl.BlockSpec(memory_space=pltpu.VMEM)
SMEM = pl.BlockSpec(memory_space=pltpu.SMEM)
ANY = pl.BlockSpec(memory_space=pl.ANY)
NT = (((1,), (1,)), ((), ()))
NN = (((1,), (0,)), ((), ()))


def wave(rows, cols, period, factor):
    angle = (np.outer(rows, cols) % period) * (2.0 * math.pi / period)
    return np.cos(angle) * factor, np.sin(angle) * factor


def first_tables(grid):
    span = grid // RADIX
    blocks = grid // 2 // RADIX
    cols = np.arange(span)

    def of(i):
        return wave(RADIX * np.arange(blocks) + i, cols, grid, grid**-0.5)

    real = []
    for i in (0, RADIX // 2):
        cos, sin = of(i)
        real.append(np.concatenate([cos, -sin], 0))
    pairs = []
    for i in range(1, RADIX // 2):
        cos, sin = of(i)
        cos_m, sin_m = of(RADIX - i)
        pairs.append(
            np.concatenate(
                [
                    np.concatenate([cos, sin], 1),
                    np.concatenate([-sin, cos], 1),
                    np.concatenate([cos_m, -sin_m], 1),
                    np.concatenate([-sin_m, -cos_m], 1),
                ],
                0,
            )
        )
    return np.stack(real).astype(jnp.bfloat16), np.stack(pairs).astype(jnp.bfloat16)


def second_tables(grid, rows):
    period = grid // WIDE
    phase = np.stack(wave(np.arange(period), np.arange(period), period, 1.0)).astype(np.float32)
    cos, sin = wave(np.arange(grid), np.arange(WIDE), grid, grid**-0.5)
    cos, sin = np.tile(cos, (1, RADIX)), np.tile(sin, (1, RADIX))
    cos, sin = cos.reshape(-1, rows, cos.shape[1]), sin.reshape(-1, rows, sin.shape[1])
    table = np.concatenate([np.concatenate([cos, -sin], 2), np.concatenate([sin, cos], 2)], 1)
    return phase, table.astype(jnp.bfloat16)


def group_index():
    return lax.axis_index("bl") * lax.axis_size("pol") + lax.axis_index("pol")


def group_device(index):
    pol = lax.axis_size("pol")
    return {"bl": lax.div(index, pol), "pol": lax.rem(index, pol)}


def halo_kernel(group, beams, sky, code, low, high, codes, send, recv, local):
    beam = lax.axis_index("beam")
    me = group_index()
    barrier = pltpu.get_barrier_semaphore()
    width = low.shape[1]
    to_next = pltpu.make_async_remote_copy(
        src_ref=sky.at[:, pl.ds(sky.shape[1] - width, width)], dst_ref=low,
        send_sem=send.at[0], recv_sem=recv.at[0],
        device_id={"beam": beam + 1}, device_id_type=MESH,
    )
    to_last = pltpu.make_async_remote_copy(
        src_ref=sky.at[:, pl.ds(0, width)], dst_ref=high,
        send_sem=send.at[1], recv_sem=recv.at[1],
        device_id={"beam": beam - 1}, device_id_type=MESH,
    )
    has_next, has_last = beam < beams - 1, beam > 0
    for step in range(1, group):
        pl.semaphore_signal(barrier, inc=1, device_id=group_device(lax.rem(me + step, group)), device_id_type=MESH)

    @pl.when(has_next)
    def _():
        pl.semaphore_signal(barrier, inc=1, device_id={"beam": beam + 1}, device_id_type=MESH)

    @pl.when(has_last)
    def _():
        pl.semaphore_signal(barrier, inc=1, device_id={"beam": beam - 1}, device_id_type=MESH)

    edges = jnp.where(beam < beams - 1, 1, 0) + jnp.where(beam > 0, 1, 0)
    pl.semaphore_wait(barrier, group - 1 + edges)

    @pl.when(has_next)
    def _():
        to_next.start()

    @pl.when(has_last)
    def _():
        to_last.start()

    copies = []
    for step in range(1, group):
        copy = pltpu.make_async_remote_copy(
            src_ref=code, dst_ref=codes.at[me],
            send_sem=send.at[1 + step], recv_sem=recv.at[1 + step],
            device_id=group_device(lax.rem(me + step, group)), device_id_type=MESH,
        )
        copy.start()
        copies.append(copy)
    own = pltpu.make_async_copy(code, codes.at[me], local)
    own.start()
    own.wait()
    for copy in copies:
        copy.wait()

    @pl.when(has_next)
    def _():
        to_next.wait_send()

    @pl.when(has_last)
    def _():
        to_last.wait_send()

    @pl.when(has_last)
    def _():
        to_next.wait_recv()

    @pl.when(has_next)
    def _():
        to_last.wait_recv()


def transform_rows(beams, image, half, pattern, sky, low, high, real_table, pair_table, g_real, g_pair, re, im):
    rows = pattern.shape[0]
    span = pattern.shape[1] // RADIX
    width = low.shape[1]
    beam = lax.axis_index("beam")
    step = 32
    root = math.sqrt(0.5)

    def fold(index, carry):
        at = pl.ds(pl.multiple_of(index * step, step), step)
        left = jnp.where(beam > 0, low[at, :], jnp.zeros((step, width), low.dtype))
        right = jnp.where(beam < beams - 1, high[at, :], jnp.zeros((step, width), high.dtype))
        window = jnp.concatenate([left, sky[at, :], right], axis=1)
        parts = []
        for a in range(RADIX):
            cut = slice(a * span, (a + 1) * span)
            weighted = pattern[at, cut].astype(jnp.float32) * window[:, cut].astype(jnp.float32)
            parts.append(weighted.astype(jnp.bfloat16).astype(jnp.float32))
        s = [parts[a] + parts[a + 4] for a in range(4)]
        d = [parts[a] - parts[a + 4] for a in range(4)]
        even, odd = s[0] + s[2], s[1] + s[3]
        near, far = root * (d[1] - d[3]), root * (d[1] + d[3])

        def put(ref, lead, off, value):
            ref[lead, at, off : off + span] = value.astype(jnp.bfloat16)

        put(g_real, 0, 0, even + odd)
        put(g_real, 1, 0, even - odd)
        put(g_pair, 0, 0, d[0] + near)
        put(g_pair, 0, span, -(d[2] + far))
        put(g_pair, 1, 0, s[0] - s[2])
        put(g_pair, 1, span, s[3] - s[1])
        put(g_pair, 2, 0, d[0] - near)
        put(g_pair, 2, span, d[2] - far)
        return carry

    lax.fori_loop(0, rows // step, fold, 0)
    blocks = re.shape[1] // RADIX
    lanes = re.shape[2]

    def place(ref, i, value):
        for k in range(ref.shape[0]):
            ref[k, pl.ds(i, blocks, stride=RADIX), :] = value[:, k * lanes : (k + 1) * lanes]

    for k, i in enumerate((0, RADIX // 2)):
        out = lax.dot_general(real_table[k], g_real[k], NT, preferred_element_type=jnp.float32)
        place(re, i, out[:blocks])
        place(im, i, out[blocks:])
    for k in range(RADIX // 2 - 1):
        out = lax.dot_general(pair_table[k], g_pair[k], NT, preferred_element_type=jnp.float32)
        for n, (ref, i) in enumerate(((re, k + 1), (im, k + 1), (re, RADIX - 1 - k), (im, RADIX - 1 - k))):
            place(ref, i, out[n * blocks : (n + 1) * blocks])


def asked_tiles(codes, phase, table, re, im, turned, part):
    group, _, lanes = codes.shape
    period = phase.shape[1]
    vis = part.shape[0] // group
    cells = RADIX * WIDE
    own = lax.broadcasted_iota(jnp.int32, (RADIX, 2 * cells), 0)
    column = lax.broadcasted_iota(jnp.int32, (RADIX, 2 * cells), 1)
    keep = own == (column % cells) // WIDE
    weights = table[group_index()]

    def one(asker, r):
        tile = codes[asker, 0, r]
        up = tile // period
        at = pl.ds(pl.multiple_of(up * RADIX, RADIX), RADIX)
        turn = tile - up * period
        cos = phase[0, pl.ds(turn, 1), :]
        sin = phase[1, pl.ds(turn, 1), :]
        real, imag = [], []
        for k in range(re.shape[0]):
            x, y = re[k, at, :], im[k, at, :]
            real.append(x * cos + y * sin)
            imag.append(y * cos - x * sin)
        return jnp.concatenate(real + imag, axis=1)

    def of_asker(asker, carry):
        def turn_pair(p, inner):
            both = jnp.concatenate([one(asker, 2 * p), one(asker, 2 * p + 1)], axis=0)
            turned[pl.ds(pl.multiple_of(p * 2 * RADIX, 2 * RADIX), 2 * RADIX), :] = both.astype(jnp.bfloat16)
            return inner

        lax.fori_loop(0, vis // 2, turn_pair, 0, unroll=4)
        cells_of = lax.dot_general(turned[...], weights, NN, preferred_element_type=jnp.float32)
        picked = jnp.where(keep[None], cells_of.reshape(vis, RADIX, 2 * cells), 0.0)
        part[pl.ds(pl.multiple_of(asker * vis, vis), vis), :] = jnp.sum(picked, axis=1).astype(part.dtype)
        return carry

    lax.fori_loop(0, group, of_asker, 0)


def tiles_kernel(
    beams, pattern, sky, low, high, codes, real_table, pair_table, phase, table, part,
    g_real, g_pair, re, im, turned,
):
    transform_rows(beams, None, None, pattern, sky, low, high, real_table, pair_table, g_real, g_pair, re, im)
    asked_tiles(codes, phase, table, re, im, turned, part)


def exchange(group, source_of, target, send, recv):
    me = group_index()
    copies = []
    for step in range(1, group):
        peer = lax.rem(me + step, group)
        copy = pltpu.make_async_remote_copy(
            src_ref=source_of(peer), dst_ref=target.at[me],
            send_sem=send.at[step - 1], recv_sem=recv.at[step - 1],
            device_id=group_device(peer), device_id_type=MESH,
        )
        copy.start()
        copies.append(copy)
    return copies


def residual_kernel(
    group, part, kernels, observed, counts, residual, shared,
    came, given, wide, narrow, send, recv, send_two, recv_two,
):
    me = group_index()
    vis = given.shape[0]
    cells = kernels.shape[1]
    barrier = pltpu.get_barrier_semaphore()
    for step in range(1, group):
        pl.semaphore_signal(barrier, inc=1, device_id=group_device(lax.rem(me + step, group)), device_id_type=MESH)
    pl.semaphore_wait(barrier, group - 1)
    first = exchange(group, lambda peer: part.at[pl.ds(pl.multiple_of(peer * vis, vis), vis)], came, send, recv)
    mine = part[pl.ds(pl.multiple_of(me * vis, vis), vis), :].astype(jnp.float32)
    wide[...] = jnp.zeros_like(wide)
    live = lax.broadcasted_iota(jnp.int32, (vis, vis), 0) == lax.broadcasted_iota(jnp.int32, (vis, vis), 1)
    count = jnp.sum(jnp.where(live, counts[...].astype(jnp.float32), 0.0), axis=1, keepdims=True)
    mask = lax.broadcasted_iota(jnp.int32, (vis, cells), 1).astype(jnp.float32) < count
    for copy in first:
        copy.wait()
    for step in range(1, group):
        mine = mine + came[lax.rem(me + step, group)].astype(jnp.float32)
    for c in range(2):
        wide[pl.ds(c, vis, stride=RADIX), :] = mine[:, c * cells : (c + 1) * cells]

    def predict(r, carry):
        at = pl.ds(pl.multiple_of(r * RADIX, RADIX), RADIX)
        narrow[at, :] = lax.dot_general(
            wide[at, :].astype(jnp.bfloat16), kernels[r], NT, preferred_element_type=jnp.float32
        )
        return carry

    lax.fori_loop(0, vis, predict, 0, unroll=8)
    for c in range(2):
        seen = observed[pl.ds(c, vis, stride=2), :]
        left = jnp.where(mask, seen - narrow[pl.ds(c, vis, stride=RADIX), :], 0.0)
        residual[pl.ds(c, vis, stride=2), :] = left
        wide[pl.ds(c, vis, stride=RADIX), :] = left

    def grid_back(r, carry):
        at = pl.ds(pl.multiple_of(r * RADIX, RADIX), RADIX)
        narrow[at, :] = lax.dot_general(
            wide[at, :].astype(jnp.bfloat16), kernels[r], NN, preferred_element_type=jnp.float32
        )
        return carry

    lax.fori_loop(0, vis, grid_back, 0, unroll=8)
    for c in range(2):
        given[:, c * cells : (c + 1) * cells] = narrow[pl.ds(c, vis, stride=RADIX), :].astype(given.dtype)
    second = exchange(group, lambda peer: given, shared, send_two, recv_two)
    shared[me] = given[...]
    for copy in second:
        copy.wait()


def dirty_kernel(keys, terms, dirty):
    rows = dirty.shape[0] // 2
    cells = dirty.shape[1]
    step = 256
    start = pl.program_id(0) * rows
    key = keys[...]

    def some(index, carry):
        tile = lax.broadcasted_iota(jnp.int32, (step, key.shape[1]), 0) + (start + index * step)
        onehot = jnp.where(tile == key, 1.0, 0.0).astype(jnp.bfloat16)
        out = lax.dot_general(onehot, terms[...], NN, preferred_element_type=jnp.float32)
        for c in range(2):
            dirty[pl.ds(index * step * 2 + c, step, stride=2), :] = out[:, c * cells : (c + 1) * cells]
        return carry

    lax.fori_loop(0, rows // step, some, 0)


def on_device(sky_model, beam_pattern, kernels, observed, tile_owner, tile_local, vis_count):
    group = lax.axis_size(("bl", "pol"))
    beams = lax.axis_size("beam")
    rows, grid = beam_pattern.shape[1:]
    strip = sky_model.shape[1]
    halo = (grid - strip) // 2
    vis, cells = kernels.shape[1], kernels.shape[3]
    tiles_all = (grid // 2 // RADIX) * (grid // WIDE)
    tiles_dev = tiles_all // group
    lanes = 128
    code = tile_owner[0, :, 0] * tiles_dev + tile_local[0]
    code = jnp.broadcast_to(jnp.pad(code, (0, lanes - vis))[None], (8, lanes))
    f32, bf16 = jnp.float32, jnp.bfloat16

    low, high, codes = pl.pallas_call(
        functools.partial(halo_kernel, group, beams),
        out_shape=(
            jax.ShapeDtypeStruct((rows, halo), bf16),
            jax.ShapeDtypeStruct((rows, halo), bf16),
            jax.ShapeDtypeStruct((group, 8, lanes), jnp.int32),
        ),
        in_specs=[ANY, ANY],
        out_specs=(ANY, ANY, ANY),
        scratch_shapes=[
            pltpu.SemaphoreType.DMA((group + 1,)),
            pltpu.SemaphoreType.DMA((group + 1,)),
            pltpu.SemaphoreType.DMA(()),
        ],
        compiler_params=pltpu.CompilerParams(collective_id=0, has_side_effects=True),
        name="halo",
    )(sky_model, code)

    real_table, pair_table = first_tables(grid)
    phase, table = second_tables(grid, rows)
    span, period = grid // RADIX, grid // WIDE
    part = pl.pallas_call(
        functools.partial(tiles_kernel, beams),
        out_shape=jax.ShapeDtypeStruct((group * vis, 2 * cells), bf16),
        in_specs=[VMEM, VMEM, VMEM, VMEM, SMEM, VMEM, VMEM, VMEM, VMEM],
        out_specs=VMEM,
        scratch_shapes=[
            pltpu.VMEM((2, rows, span), bf16),
            pltpu.VMEM((RADIX // 2 - 1, rows, 2 * span), bf16),
            pltpu.VMEM((rows // period, grid // 2, period), f32),
            pltpu.VMEM((rows // period, grid // 2, period), f32),
            pltpu.VMEM((vis * RADIX, 2 * rows), bf16),
        ],
        compiler_params=pltpu.CompilerParams(vmem_limit_bytes=48 * 1024 * 1024),
        name="tiles",
    )(
        beam_pattern[0], sky_model, low, high, codes,
        jnp.asarray(real_table), jnp.asarray(pair_table), jnp.asarray(phase), jnp.asarray(table),
    )

    residual, shared = pl.pallas_call(
        functools.partial(residual_kernel, group),
        out_shape=(
            jax.ShapeDtypeStruct((vis * 2, cells), f32),
            jax.ShapeDtypeStruct((group, vis, 2 * cells), bf16),
        ),
        in_specs=[VMEM] * 4,
        out_specs=(VMEM, VMEM),
        scratch_shapes=[
            pltpu.VMEM((group, vis, 2 * cells), bf16),
            pltpu.VMEM((vis, 2 * cells), bf16),
            pltpu.VMEM((vis * RADIX, cells), f32),
            pltpu.VMEM((vis * RADIX, cells), f32),
            pltpu.SemaphoreType.DMA((group - 1,)),
            pltpu.SemaphoreType.DMA((group - 1,)),
            pltpu.SemaphoreType.DMA((group - 1,)),
            pltpu.SemaphoreType.DMA((group - 1,)),
        ],
        compiler_params=pltpu.CompilerParams(collective_id=1, has_side_effects=True),
        name="residual",
    )(part, kernels[0], observed.reshape(vis * 2, cells), vis_count)

    keys = codes[:, 0, :vis].reshape(1, group * vis) - group_index() * tiles_dev
    blocks = 4
    dirty = pl.pallas_call(
        dirty_kernel,
        grid=(blocks,),
        out_shape=jax.ShapeDtypeStruct((tiles_dev * 2, cells), f32),
        in_specs=[
            pl.BlockSpec((1, group * vis), lambda i: (0, 0)),
            pl.BlockSpec((group * vis, 2 * cells), lambda i: (0, 0)),
        ],
        out_specs=pl.BlockSpec((tiles_dev * 2 // blocks, cells), lambda i: (i, 0)),
        name="dirty",
    )(keys, shared.reshape(group * vis, 2 * cells))
    return (
        residual.reshape(1, vis, 2, cells),
        dirty.reshape(1, tiles_dev, 2, cells),
    )


def solution(mesh):
    placed = (
        P(("tile", "bl", "pol"), "beam"),
        P(("tile", "beam"), ("bl", "pol"), None),
        P(("tile", "beam"), ("bl", "pol"), None, None),
        P(("tile", "beam"), ("bl", "pol"), None, None),
        P(("tile", "beam"), ("bl", "pol"), None),
        P(("tile", "beam"), ("bl", "pol")),
        P(("tile", "beam"), ("bl", "pol")),
    )
    return jax.shard_map(
        on_device,
        mesh=mesh,
        in_specs=placed,
        out_specs=(
            P(("tile", "beam"), ("bl", "pol"), None, None),
            P(("tile", "beam"), ("bl", "pol"), None, None),
        ),
        check_vma=False,
    )
```

```python
import functools
import math

import jax
import jax.numpy as jnp
import numpy as np
from jax import lax
from jax.experimental import pallas as pl
from jax.experimental.pallas import tpu as pltpu
from jax.sharding import PartitionSpec as P

MESH = pl.DeviceIdType.MESH
RADIX = 8
WIDE = 16
VMEM = pl.BlockSpec(memory_space=pltpu.VMEM)
HBM = pl.BlockSpec(memory_space=pltpu.HBM)
NT = (((1,), (1,)), ((), ()))
NN = (((1,), (0,)), ((), ()))


def wave(rows, cols, period, factor):
    angle = (np.outer(rows, cols) % period) * (2.0 * math.pi / period)
    return np.cos(angle) * factor, np.sin(angle) * factor


def first_tables(grid):
    span = grid // RADIX
    blocks = grid // 2 // RADIX
    cols = np.arange(span)

    def of(i):
        return wave(RADIX * np.arange(blocks) + i, cols, grid, grid**-0.5)

    real = []
    for i in (0, RADIX // 2):
        cos, sin = of(i)
        real.append(np.concatenate([cos, -sin], 0))
    pairs = []
    for i in range(1, RADIX // 2):
        cos, sin = of(i)
        cos_m, sin_m = of(RADIX - i)
        pairs.append(
            np.concatenate(
                [
                    np.concatenate([cos, sin], 1),
                    np.concatenate([-sin, cos], 1),
                    np.concatenate([cos_m, -sin_m], 1),
                    np.concatenate([-sin_m, -cos_m], 1),
                ],
                0,
            )
        )
    return np.stack(real).astype(jnp.bfloat16), np.stack(pairs).astype(jnp.bfloat16)


def second_tables(grid):
    period = grid // WIDE
    phase = np.stack(wave(np.arange(period), np.arange(period), period, 1.0), 1).astype(np.float32)
    cos, sin = wave(np.arange(grid), np.arange(WIDE), grid, grid**-0.5)
    cos, sin = np.tile(cos, (1, RADIX)), np.tile(sin, (1, RADIX))
    cos, sin = cos.reshape(-1, period, cos.shape[1]), sin.reshape(-1, period, sin.shape[1])
    table = np.concatenate([np.concatenate([cos, -sin], 2), np.concatenate([sin, cos], 2)], 1)
    return phase, table.astype(jnp.bfloat16)


def group_index():
    return lax.axis_index("bl") * lax.axis_size("pol") + lax.axis_index("pol")


def group_device(index):
    pol = lax.axis_size("pol")
    return {"bl": lax.div(index, pol), "pol": lax.rem(index, pol)}


def transform_rows(beams, at, pattern, strip, low, high, real_table, pair_table, g_real, g_pair, re, im):
    span = pattern.shape[1] // RADIX
    width = low.shape[1]
    beam = lax.axis_index("beam")
    step = 32
    root = math.sqrt(0.5)

    def fold(index, carry):
        src = pl.ds(pl.multiple_of(at + index * step, step), step)
        dst = pl.ds(pl.multiple_of(index * step, step), step)
        left = jnp.where(beam > 0, low[src, :], jnp.zeros((step, width), low.dtype))
        right = jnp.where(beam < beams - 1, high[src, :], jnp.zeros((step, width), high.dtype))
        window = jnp.concatenate([left, strip[src, :], right], axis=1)
        parts = []
        for a in range(RADIX):
            cut = slice(a * span, (a + 1) * span)
            weighted = pattern[src, cut].astype(jnp.float32) * window[:, cut].astype(jnp.float32)
            parts.append(weighted.astype(jnp.bfloat16).astype(jnp.float32))
        s = [parts[a] + parts[a + 4] for a in range(4)]
        d = [parts[a] - parts[a + 4] for a in range(4)]
        even, odd = s[0] + s[2], s[1] + s[3]
        near, far = root * (d[1] - d[3]), root * (d[1] + d[3])

        def put(ref, lead, off, value):
            ref[lead, dst, off : off + span] = value.astype(jnp.bfloat16)

        put(g_real, 0, 0, even + odd)
        put(g_real, 1, 0, even - odd)
        put(g_pair, 0, 0, d[0] + near)
        put(g_pair, 0, span, -(d[2] + far))
        put(g_pair, 1, 0, s[0] - s[2])
        put(g_pair, 1, span, s[3] - s[1])
        put(g_pair, 2, 0, d[0] - near)
        put(g_pair, 2, span, d[2] - far)
        return carry

    lax.fori_loop(0, g_real.shape[1] // step, fold, 0)
    blocks = re.shape[0]
    re = re.reshape(blocks * RADIX, re.shape[2])
    im = im.reshape(blocks * RADIX, im.shape[2])
    for k, i in enumerate((0, RADIX // 2)):
        out = lax.dot_general(real_table[k], g_real[k], NT, preferred_element_type=jnp.float32)
        re[pl.ds(i, blocks, stride=RADIX), :] = out[:blocks]
        im[pl.ds(i, blocks, stride=RADIX), :] = out[blocks:]
    for k in range(RADIX // 2 - 1):
        out = lax.dot_general(pair_table[k], g_pair[k], NT, preferred_element_type=jnp.float32)
        for n, (ref, i) in enumerate(((re, k + 1), (im, k + 1), (re, RADIX - 1 - k), (im, RADIX - 1 - k))):
            ref[pl.ds(i, blocks, stride=RADIX), :] = out[n * blocks : (n + 1) * blocks]


def asked_tiles(asker, codes, phase, weights, re, im, turned):
    period = phase.shape[2]
    vis = turned.shape[0] // RADIX
    cells = RADIX * WIDE
    own = lax.broadcasted_iota(jnp.int32, (RADIX, 2 * cells), 0)
    column = lax.broadcasted_iota(jnp.int32, (RADIX, 2 * cells), 1)
    keep = own == (column % cells) // WIDE

    def one(r):
        tile = codes[asker, 0, r]
        turn = phase[lax.rem(tile, period)]
        cos, sin = turn[0:1], turn[1:2]
        up = lax.div(tile, period)
        x, y = re[up], im[up]
        return jnp.concatenate([x * cos + y * sin, y * cos - x * sin], axis=1)

    def turn_pair(p, carry):
        both = jnp.concatenate([one(2 * p), one(2 * p + 1)], axis=0)
        turned[pl.ds(pl.multiple_of(p * 2 * RADIX, 2 * RADIX), 2 * RADIX), :] = both.astype(jnp.bfloat16)
        return carry

    lax.fori_loop(0, vis // 2, turn_pair, 0, unroll=8)
    cells_of = lax.dot_general(turned[...], weights, NN, preferred_element_type=jnp.float32)
    picked = jnp.where(keep[None], cells_of.reshape(vis, RADIX, 2 * cells), 0.0)
    return jnp.sum(picked, axis=1)


def predict_kernel(
    group, beams, tiles_dev,
    sky, pattern_in, kernels_in, observed, owner, place, counts, real_in, pair_in, phase_in, table_in,
    residual, shared, codes,
    strip, low, high, pattern, kernels, real_table, pair_table, phase, table, code, codes_s,
    g_real, g_pair, re, im, turned, total, part, came, given, wide, narrow,
    local, halo_send, halo_recv, code_send, code_recv, part_send, part_recv, share_send, share_recv,
):
    beam = lax.axis_index("beam")
    me = group_index()
    vis, cells = kernels.shape[0], kernels.shape[1]
    width = low.shape[1]
    period = phase.shape[2]
    chunks = pattern.shape[0] // period

    loads = []
    for n, (src, dst) in enumerate((
        (pattern_in, pattern), (sky, strip), (real_in, real_table), (pair_in, pair_table), (phase_in, phase),
        (table_in.at[pl.ds(me * chunks, chunks)], table), (kernels_in, kernels),
    )):
        load = pltpu.make_async_copy(src, dst, local.at[n])
        load.start()
        loads.append(load)

    named = jnp.broadcast_to(owner[...] * tiles_dev + place[...], (code.shape[0], vis))
    for n in range(code.shape[1] // vis):
        code[:, n * vis : (n + 1) * vis] = named

    barrier = pltpu.get_barrier_semaphore()
    has_next, has_last = beam < beams - 1, beam > 0

    def greet(device):
        pl.semaphore_signal(barrier, inc=1, device_id=device, device_id_type=MESH)

    for step in range(1, group):
        greet(group_device(lax.rem(me + step, group)))

    @pl.when(has_next)
    def _():
        greet({"beam": beam + 1})

    @pl.when(has_last)
    def _():
        greet({"beam": beam - 1})

    edges = jnp.where(beam < beams - 1, 1, 0) + jnp.where(beam > 0, 1, 0)
    pl.semaphore_wait(barrier, group - 1 + edges)

    def halo(side, k):
        rows = pl.ds(pl.multiple_of(k * period, period), period)
        first = 0 if side else sky.shape[1] - width
        return pltpu.make_async_remote_copy(
            src_ref=sky.at[rows, pl.ds(first, width)], dst_ref=(high if side else low).at[rows, :],
            send_sem=halo_send.at[side, k], recv_sem=halo_recv.at[side, k],
            device_id={"beam": beam - 1 if side else beam + 1}, device_id_type=MESH,
        )

    def to_peer(step, source, target, send, recv):
        return pltpu.make_async_remote_copy(
            src_ref=source, dst_ref=target,
            send_sem=send.at[step - 1], recv_sem=recv.at[step - 1],
            device_id=group_device(lax.rem(me + step, group)), device_id_type=MESH,
        )

    @pl.when(has_next)
    def _():
        for k in range(chunks):
            halo(0, k).start()

    @pl.when(has_last)
    def _():
        for k in range(chunks):
            halo(1, k).start()

    named_copies = [to_peer(step, code, codes.at[me], code_send, code_recv) for step in range(1, group)]
    for copy in named_copies:
        copy.start()
    codes[me] = code[...]
    total[...] = jnp.zeros_like(total)
    wide[...] = jnp.zeros_like(wide)
    for copy in named_copies:
        copy.wait()
    to_scalar = pltpu.make_async_copy(codes, codes_s, local.at[len(loads)])
    to_scalar.start()
    to_scalar.wait()
    for load in loads[:-1]:
        load.wait()

    def of_chunk(k, carry):
        @pl.when(has_last)
        def _():
            halo(0, k).wait_recv()

        @pl.when(has_next)
        def _():
            halo(1, k).wait_recv()

        transform_rows(
            beams, k * period, pattern, strip, low, high, real_table, pair_table, g_real, g_pair, re, im
        )

        def of_asker(step, inner):
            asker = lax.rem(me + step, group)
            rows = pl.ds(pl.multiple_of(asker * vis, vis), vis)
            total[rows, :] += asked_tiles(asker, codes_s, phase, table[k], re, im, turned)

            @pl.when((k == chunks - 1) & (step < group))
            def _():
                part[rows, :] = total[rows, :].astype(part.dtype)
                to_peer(step, part.at[rows, :], came.at[me], part_send, part_recv).start()

            return inner

        lax.fori_loop(1, group + 1, of_asker, 0)
        return carry

    lax.fori_loop(0, chunks, of_chunk, 0)

    own = lax.broadcasted_iota(jnp.int32, (vis, vis), 0) == lax.broadcasted_iota(jnp.int32, (vis, vis), 1)
    count = jnp.sum(jnp.where(own, counts[...].astype(jnp.float32), 0.0), axis=1, keepdims=True)
    mask = lax.broadcasted_iota(jnp.int32, (vis, cells), 1).astype(jnp.float32) < count
    mine = total[pl.ds(pl.multiple_of(me * vis, vis), vis), :]
    loads[-1].wait()
    for step in range(1, group):
        rows = pl.ds(pl.multiple_of(lax.rem(me + step, group) * vis, vis), vis)
        to_peer(step, part.at[rows, :], came.at[me], part_send, part_recv).wait()
    for step in range(1, group):
        mine = mine + came[lax.rem(me + step, group)].astype(jnp.float32)
    for c in range(2):
        wide[pl.ds(c, vis, stride=RADIX), :] = mine[:, c * cells : (c + 1) * cells]

    def apply(dims):
        def of_tile(r, carry):
            at = pl.ds(pl.multiple_of(r * RADIX, RADIX), RADIX)
            narrow[at, :] = lax.dot_general(
                wide[at, :].astype(jnp.bfloat16), kernels[r], dims, preferred_element_type=jnp.float32
            )
            return carry

        lax.fori_loop(0, vis, of_tile, 0, unroll=16)

    apply(NT)
    for c in range(2):
        seen = observed[pl.ds(c, vis, stride=2), :]
        left = jnp.where(mask, seen - narrow[pl.ds(c, vis, stride=RADIX), :], 0.0)
        residual[pl.ds(c, vis, stride=2), :] = left
        wide[pl.ds(c, vis, stride=RADIX), :] = left
    apply(NN)
    for c in range(2):
        given[:, c * cells : (c + 1) * cells] = narrow[pl.ds(c, vis, stride=RADIX), :].astype(given.dtype)
    given_copies = [to_peer(step, given, shared.at[me], share_send, share_recv) for step in range(1, group)]
    for copy in given_copies:
        copy.start()
    shared[me] = given[...]
    for copy in given_copies:
        copy.wait()

    @pl.when(has_next)
    def _():
        for k in range(chunks):
            halo(0, k).wait_send()

    @pl.when(has_last)
    def _():
        for k in range(chunks):
            halo(1, k).wait_send()


def dirty_kernel(vis, codes, terms, dirty):
    rows = dirty.shape[0] // 2
    cells = dirty.shape[1]
    group, _, lanes = codes.shape
    start = pl.program_id(0) * rows + group_index() * rows * pl.num_programs(0)
    each = lanes // vis
    lane = lax.broadcasted_iota(jnp.int32, (1, lanes), 1)
    keys = []
    for first in range(0, group, each):
        key = codes[first, 0:1, :]
        for n in range(1, each):
            key = jnp.where(lane < n * vis, key, codes[first + n, 0:1, :])
        keys.append(key)
    key = jnp.concatenate(keys, axis=1) - start
    tile = lax.broadcasted_iota(jnp.int32, (rows, key.shape[1]), 0)
    onehot = jnp.where(tile == key, 1.0, 0.0).astype(jnp.bfloat16)
    out = lax.dot_general(onehot, terms[...], NN, preferred_element_type=jnp.float32)
    for c in range(2):
        dirty[pl.ds(c, rows, stride=2), :] = out[:, c * cells : (c + 1) * cells]


def on_device(sky_model, beam_pattern, kernels, observed, tile_owner, tile_local, vis_count):
    group = lax.axis_size(("bl", "pol"))
    beams = lax.axis_size("beam")
    rows, grid = beam_pattern.shape[1:]
    strip = sky_model.shape[1]
    halo = (grid - strip) // 2
    vis, cells = kernels.shape[1], kernels.shape[3]
    tiles_dev = (grid // 2 // RADIX) * (grid // WIDE) // group
    lanes = 128
    f32, bf16 = jnp.float32, jnp.bfloat16
    real_table, pair_table = first_tables(grid)
    phase, table = second_tables(grid)
    span, period = grid // RADIX, grid // WIDE
    chunks = rows // period
    dma = pltpu.SemaphoreType.DMA

    residual, shared, codes = pl.pallas_call(
        functools.partial(predict_kernel, group, beams, tiles_dev),
        out_shape=(
            jax.ShapeDtypeStruct((vis * 2, cells), f32),
            jax.ShapeDtypeStruct((group, vis, 2 * cells), bf16),
            jax.ShapeDtypeStruct((group, 8, lanes), jnp.int32),
        ),
        in_specs=[HBM, HBM, HBM, VMEM, VMEM, VMEM, VMEM, HBM, HBM, HBM, HBM],
        out_specs=(VMEM, VMEM, VMEM),
        scratch_shapes=[
            pltpu.VMEM((rows, strip), bf16),
            pltpu.VMEM((rows, halo), bf16),
            pltpu.VMEM((rows, halo), bf16),
            pltpu.VMEM((rows, grid), bf16),
            pltpu.VMEM((vis, cells, cells), bf16),
            pltpu.VMEM(real_table.shape, bf16),
            pltpu.VMEM(pair_table.shape, bf16),
            pltpu.VMEM(phase.shape, f32),
            pltpu.VMEM((chunks, *table.shape[1:]), bf16),
            pltpu.VMEM((8, lanes), jnp.int32),
            pltpu.SMEM((group, 8, lanes), jnp.int32),
            pltpu.VMEM((2, period, span), bf16),
            pltpu.VMEM((RADIX // 2 - 1, period, 2 * span), bf16),
            pltpu.VMEM((grid // 2 // RADIX, RADIX, period), f32),
            pltpu.VMEM((grid // 2 // RADIX, RADIX, period), f32),
            pltpu.VMEM((vis * RADIX, 2 * period), bf16),
            pltpu.VMEM((group * vis, 2 * cells), f32),
            pltpu.VMEM((group * vis, 2 * cells), bf16),
            pltpu.VMEM((group, vis, 2 * cells), bf16),
            pltpu.VMEM((vis, 2 * cells), bf16),
            pltpu.VMEM((vis * RADIX, cells), f32),
            pltpu.VMEM((vis * RADIX, cells), f32),
            dma((8,)),
            dma((2, chunks)), dma((2, chunks)),
            dma((group - 1,)), dma((group - 1,)),
            dma((group - 1,)), dma((group - 1,)),
            dma((group - 1,)), dma((group - 1,)),
        ],
        compiler_params=pltpu.CompilerParams(
            collective_id=0, has_side_effects=True, vmem_limit_bytes=60 * 1024 * 1024
        ),
        name="predict",
    )(
        sky_model, beam_pattern[0], kernels[0], observed.reshape(vis * 2, cells),
        tile_owner.reshape(1, vis), tile_local, vis_count,
        jnp.asarray(real_table), jnp.asarray(pair_table), jnp.asarray(phase), jnp.asarray(table),
    )

    blocks = 8
    dirty = pl.pallas_call(
        functools.partial(dirty_kernel, vis),
        grid=(blocks,),
        out_shape=jax.ShapeDtypeStruct((tiles_dev * 2, cells), f32),
        in_specs=[
            pl.BlockSpec(codes.shape, lambda i: (0, 0, 0)),
            pl.BlockSpec((group * vis, 2 * cells), lambda i: (0, 0)),
        ],
        out_specs=pl.BlockSpec((tiles_dev * 2 // blocks, cells), lambda i: (i, 0)),
        name="dirty",
    )(codes, shared.reshape(group * vis, 2 * cells))
    return (
        residual.reshape(1, vis, 2, cells),
        dirty.reshape(1, tiles_dev, 2, cells),
    )


def solution(mesh):
    placed = (
        P(("tile", "bl", "pol"), "beam"),
        P(("tile", "beam"), ("bl", "pol"), None),
        P(("tile", "beam"), ("bl", "pol"), None, None),
        P(("tile", "beam"), ("bl", "pol"), None, None),
        P(("tile", "beam"), ("bl", "pol"), None),
        P(("tile", "beam"), ("bl", "pol")),
        P(("tile", "beam"), ("bl", "pol")),
    )
    return jax.shard_map(
        on_device,
        mesh=mesh,
        in_specs=placed,
        out_specs=(
            P(("tile", "beam"), ("bl", "pol"), None, None),
            P(("tile", "beam"), ("bl", "pol"), None, None),
        ),
        check_vma=False,
    )
```

```python
import functools
import math

import jax
import jax.numpy as jnp
import numpy as np
from jax import lax
from jax.experimental import pallas as pl
from jax.experimental.pallas import tpu as pltpu
from jax.sharding import PartitionSpec as P

MESH = pl.DeviceIdType.MESH
RADIX = 8
WIDE = 16
VMEM = pl.BlockSpec(memory_space=pltpu.VMEM)
HBM = pl.BlockSpec(memory_space=pltpu.HBM)
NT = (((1,), (1,)), ((), ()))
NN = (((1,), (0,)), ((), ()))


def wave(rows, cols, period, factor):
    angle = (np.outer(rows, cols) % period) * (2.0 * math.pi / period)
    return np.cos(angle) * factor, np.sin(angle) * factor


def first_tables(grid):
    span = grid // RADIX
    blocks = grid // 2 // RADIX
    cols = np.arange(span)

    def of(i):
        return wave(RADIX * np.arange(blocks) + i, cols, grid, grid**-0.5)

    real = []
    for i in (0, RADIX // 2):
        cos, sin = of(i)
        real.append(np.concatenate([cos, -sin], 0))
    pairs = []
    for i in range(1, RADIX // 2):
        cos, sin = of(i)
        cos_m, sin_m = of(RADIX - i)
        pairs.append(
            np.concatenate(
                [
                    np.concatenate([cos, sin], 1),
                    np.concatenate([-sin, cos], 1),
                    np.concatenate([cos_m, -sin_m], 1),
                    np.concatenate([-sin_m, -cos_m], 1),
                ],
                0,
            )
        )
    return np.stack(real).astype(jnp.bfloat16), np.stack(pairs).astype(jnp.bfloat16)


def second_tables(grid):
    period = grid // WIDE
    phase = np.stack(wave(np.arange(period), np.arange(period), period, 1.0), 1).astype(np.float32)
    cos, sin = wave(np.arange(grid), np.arange(WIDE), grid, grid**-0.5)
    cos, sin = np.tile(cos, (1, RADIX)), np.tile(sin, (1, RADIX))
    cos, sin = cos.reshape(-1, period, cos.shape[1]), sin.reshape(-1, period, sin.shape[1])
    table = np.concatenate([np.concatenate([cos, -sin], 2), np.concatenate([sin, cos], 2)], 1)
    return phase, table.astype(jnp.bfloat16)


def group_index():
    return lax.axis_index("bl") * lax.axis_size("pol") + lax.axis_index("pol")


def group_device(index):
    pol = lax.axis_size("pol")
    return {"bl": lax.div(index, pol), "pol": lax.rem(index, pol)}


def transform_rows(beams, at, pattern, strip, low, high, real_table, pair_table, g_real, g_pair, re, im):
    span = pattern.shape[1] // RADIX
    width = low.shape[1]
    beam = lax.axis_index("beam")
    step = 32
    root = math.sqrt(0.5)

    def fold(index, carry):
        src = pl.ds(pl.multiple_of(at + index * step, step), step)
        dst = pl.ds(pl.multiple_of(index * step, step), step)
        left = jnp.where(beam > 0, low[src, :], jnp.zeros((step, width), low.dtype))
        right = jnp.where(beam < beams - 1, high[src, :], jnp.zeros((step, width), high.dtype))
        window = jnp.concatenate([left, strip[src, :], right], axis=1)
        parts = []
        for a in range(RADIX):
            cut = slice(a * span, (a + 1) * span)
            weighted = pattern[src, cut].astype(jnp.float32) * window[:, cut].astype(jnp.float32)
            parts.append(weighted.astype(jnp.bfloat16).astype(jnp.float32))
        s = [parts[a] + parts[a + 4] for a in range(4)]
        d = [parts[a] - parts[a + 4] for a in range(4)]
        even, odd = s[0] + s[2], s[1] + s[3]
        near, far = root * (d[1] - d[3]), root * (d[1] + d[3])

        def put(ref, lead, off, value):
            ref[lead, dst, off : off + span] = value.astype(jnp.bfloat16)

        put(g_real, 0, 0, even + odd)
        put(g_real, 1, 0, even - odd)
        put(g_pair, 0, 0, d[0] + near)
        put(g_pair, 0, span, -(d[2] + far))
        put(g_pair, 1, 0, s[0] - s[2])
        put(g_pair, 1, span, s[3] - s[1])
        put(g_pair, 2, 0, d[0] - near)
        put(g_pair, 2, span, d[2] - far)
        return carry

    lax.fori_loop(0, g_real.shape[1] // step, fold, 0)
    blocks = re.shape[0]
    re = re.reshape(blocks * RADIX, re.shape[2])
    im = im.reshape(blocks * RADIX, im.shape[2])
    for k, i in enumerate((0, RADIX // 2)):
        out = lax.dot_general(real_table[k], g_real[k], NT, preferred_element_type=jnp.float32)
        re[pl.ds(i, blocks, stride=RADIX), :] = out[:blocks]
        im[pl.ds(i, blocks, stride=RADIX), :] = out[blocks:]
    for k in range(RADIX // 2 - 1):
        out = lax.dot_general(pair_table[k], g_pair[k], NT, preferred_element_type=jnp.float32)
        for n, (ref, i) in enumerate(((re, k + 1), (im, k + 1), (re, RADIX - 1 - k), (im, RADIX - 1 - k))):
            ref[pl.ds(i, blocks, stride=RADIX), :] = out[n * blocks : (n + 1) * blocks]


def asked_tiles(asker, codes, phase, weights, re, im, turned):
    period = phase.shape[2]
    vis = turned.shape[0] // RADIX
    cells = RADIX * WIDE
    own = lax.broadcasted_iota(jnp.int32, (RADIX, 2 * cells), 0)
    column = lax.broadcasted_iota(jnp.int32, (RADIX, 2 * cells), 1)
    keep = own == (column % cells) // WIDE

    def one(r):
        tile = codes[asker, 0, r]
        turn = phase[jnp.bitwise_and(tile, period - 1)]
        cos, sin = turn[0:1], turn[1:2]
        up = lax.shift_right_logical(tile, period.bit_length() - 1)
        x, y = re[up], im[up]
        return jnp.concatenate([x * cos + y * sin, y * cos - x * sin], axis=1)

    def turn_pair(p, carry):
        both = jnp.concatenate([one(2 * p), one(2 * p + 1)], axis=0)
        turned[pl.ds(pl.multiple_of(p * 2 * RADIX, 2 * RADIX), 2 * RADIX), :] = both.astype(jnp.bfloat16)
        return carry

    lax.fori_loop(0, vis // 2, turn_pair, 0, unroll=8)
    cells_of = lax.dot_general(turned[...], weights, NN, preferred_element_type=jnp.float32)
    picked = jnp.where(keep[None], cells_of.reshape(vis, RADIX, 2 * cells), 0.0)
    return jnp.sum(picked, axis=1)


def predict_kernel(
    group, beams, tiles_dev,
    sky, pattern_in, kernels_in, observed, owner, place, counts, real_in, pair_in, phase_in, table_in,
    residual, shared, codes,
    strip, low, high, pattern, kernels, real_table, pair_table, phase, table, code, codes_s,
    g_real, g_pair, re, im, turned, total, part, came, given, wide, narrow,
    local, halo_send, halo_recv, code_send, code_recv, part_send, part_recv, share_send, share_recv,
):
    beam = lax.axis_index("beam")
    me = group_index()
    vis, cells = kernels.shape[0], kernels.shape[1]
    width = low.shape[1]
    period = phase.shape[2]
    chunks = pattern.shape[0] // period

    loads = []
    for n, (src, dst) in enumerate((
        (pattern_in, pattern), (sky, strip), (real_in, real_table), (pair_in, pair_table), (phase_in, phase),
        (table_in.at[pl.ds(me * chunks, chunks)], table), (kernels_in, kernels),
    )):
        load = pltpu.make_async_copy(src, dst, local.at[n])
        load.start()
        loads.append(load)

    named = jnp.broadcast_to(owner[...] * tiles_dev + place[...], (code.shape[0], vis))
    for n in range(code.shape[1] // vis):
        code[:, n * vis : (n + 1) * vis] = named

    barrier = pltpu.get_barrier_semaphore()
    has_next, has_last = beam < beams - 1, beam > 0

    def greet(device):
        pl.semaphore_signal(barrier, inc=1, device_id=device, device_id_type=MESH)

    for step in range(1, group):
        greet(group_device(lax.rem(me + step, group)))

    @pl.when(has_next)
    def _():
        greet({"beam": beam + 1})

    @pl.when(has_last)
    def _():
        greet({"beam": beam - 1})

    edges = jnp.where(beam < beams - 1, 1, 0) + jnp.where(beam > 0, 1, 0)
    pl.semaphore_wait(barrier, group - 1 + edges)

    def halo(side, k):
        rows = pl.ds(pl.multiple_of(k * period, period), period)
        first = 0 if side else sky.shape[1] - width
        return pltpu.make_async_remote_copy(
            src_ref=sky.at[rows, pl.ds(first, width)], dst_ref=(high if side else low).at[rows, :],
            send_sem=halo_send.at[side, k], recv_sem=halo_recv.at[side, k],
            device_id={"beam": beam - 1 if side else beam + 1}, device_id_type=MESH,
        )

    def to_peer(step, source, target, send, recv):
        return pltpu.make_async_remote_copy(
            src_ref=source, dst_ref=target,
            send_sem=send.at[step - 1], recv_sem=recv.at[step - 1],
            device_id=group_device(lax.rem(me + step, group)), device_id_type=MESH,
        )

    @pl.when(has_next)
    def _():
        for k in range(chunks):
            halo(0, k).start()

    @pl.when(has_last)
    def _():
        for k in range(chunks):
            halo(1, k).start()

    named_copies = [to_peer(step, code, codes.at[me], code_send, code_recv) for step in range(1, group)]
    for copy in named_copies:
        copy.start()
    codes[me] = code[...]
    total[...] = jnp.zeros_like(total)
    wide[...] = jnp.zeros_like(wide)
    for copy in named_copies:
        copy.wait()
    to_scalar = pltpu.make_async_copy(codes, codes_s, local.at[len(loads)])
    to_scalar.start()
    to_scalar.wait()
    for load in loads[:-1]:
        load.wait()

    def of_chunk(k, carry):
        @pl.when(has_last)
        def _():
            halo(0, k).wait_recv()

        @pl.when(has_next)
        def _():
            halo(1, k).wait_recv()

        transform_rows(
            beams, k * period, pattern, strip, low, high, real_table, pair_table, g_real, g_pair, re, im
        )

        def of_asker(step, inner):
            asker = lax.rem(me + step, group)
            rows = pl.ds(pl.multiple_of(asker * vis, vis), vis)
            total[rows, :] += asked_tiles(asker, codes_s, phase, table[k], re, im, turned)

            @pl.when((k == chunks - 1) & (step < group))
            def _():
                part[rows, :] = total[rows, :].astype(part.dtype)
                to_peer(step, part.at[rows, :], came.at[me], part_send, part_recv).start()

            return inner

        lax.fori_loop(1, group + 1, of_asker, 0)
        return carry

    lax.fori_loop(0, chunks, of_chunk, 0)

    own = lax.broadcasted_iota(jnp.int32, (vis, vis), 0) == lax.broadcasted_iota(jnp.int32, (vis, vis), 1)
    count = jnp.sum(jnp.where(own, counts[...].astype(jnp.float32), 0.0), axis=1, keepdims=True)
    mask = lax.broadcasted_iota(jnp.int32, (vis, cells), 1).astype(jnp.float32) < count
    mine = total[pl.ds(pl.multiple_of(me * vis, vis), vis), :]
    loads[-1].wait()
    for step in range(1, group):
        rows = pl.ds(pl.multiple_of(lax.rem(me + step, group) * vis, vis), vis)
        to_peer(step, part.at[rows, :], came.at[me], part_send, part_recv).wait()
    for step in range(1, group):
        mine = mine + came[lax.rem(me + step, group)].astype(jnp.float32)
    for c in range(2):
        wide[pl.ds(c, vis, stride=RADIX), :] = mine[:, c * cells : (c + 1) * cells]

    def apply(dims):
        def of_tile(r, carry):
            at = pl.ds(pl.multiple_of(r * RADIX, RADIX), RADIX)
            narrow[at, :] = lax.dot_general(
                wide[at, :].astype(jnp.bfloat16), kernels[r], dims, preferred_element_type=jnp.float32
            )
            return carry

        lax.fori_loop(0, vis, of_tile, 0, unroll=16)

    apply(NT)
    for c in range(2):
        seen = observed[pl.ds(c, vis, stride=2), :]
        left = jnp.where(mask, seen - narrow[pl.ds(c, vis, stride=RADIX), :], 0.0)
        residual[pl.ds(c, vis, stride=2), :] = left
        wide[pl.ds(c, vis, stride=RADIX), :] = left
    apply(NN)
    for c in range(2):
        given[:, c * cells : (c + 1) * cells] = narrow[pl.ds(c, vis, stride=RADIX), :].astype(given.dtype)
    given_copies = [to_peer(step, given, shared.at[me], share_send, share_recv) for step in range(1, group)]
    for copy in given_copies:
        copy.start()
    shared[me] = given[...]
    for copy in given_copies:
        copy.wait()

    @pl.when(has_next)
    def _():
        for k in range(chunks):
            halo(0, k).wait_send()

    @pl.when(has_last)
    def _():
        for k in range(chunks):
            halo(1, k).wait_send()


def dirty_kernel(vis, codes, terms, left, dirty, residual, held, sems):
    blocks, rows, cells = held.shape
    rows = rows // 2
    group, _, lanes = codes.shape
    start = group_index() * rows * blocks
    residual[...] = left[...]
    each = lanes // vis
    lane = lax.broadcasted_iota(jnp.int32, (1, lanes), 1)
    keys = []
    for first in range(0, group, each):
        key = codes[first, 0:1, :]
        for n in range(1, each):
            key = jnp.where(lane < n * vis, key, codes[first + n, 0:1, :])
        keys.append(key)
    key = jnp.concatenate(keys, axis=1) - start
    tile = lax.broadcasted_iota(jnp.int32, (rows, key.shape[1]), 0)
    copies = []
    for block in range(blocks):
        onehot = jnp.where(tile == key - block * rows, 1.0, 0.0).astype(jnp.bfloat16)
        out = lax.dot_general(onehot, terms[...], NN, preferred_element_type=jnp.float32)
        for c in range(2):
            held[block, pl.ds(c, rows, stride=2), :] = out[:, c * cells : (c + 1) * cells]
        copy = pltpu.make_async_copy(
            held.at[block], dirty.at[pl.ds(block * rows * 2, rows * 2), :], sems.at[block]
        )
        copy.start()
        copies.append(copy)
    for copy in copies:
        copy.wait()


def on_device(sky_model, beam_pattern, kernels, observed, tile_owner, tile_local, vis_count):
    group = lax.axis_size(("bl", "pol"))
    beams = lax.axis_size("beam")
    rows, grid = beam_pattern.shape[1:]
    strip = sky_model.shape[1]
    halo = (grid - strip) // 2
    vis, cells = kernels.shape[1], kernels.shape[3]
    tiles_dev = (grid // 2 // RADIX) * (grid // WIDE) // group
    lanes = 128
    f32, bf16 = jnp.float32, jnp.bfloat16
    real_table, pair_table = first_tables(grid)
    phase, table = second_tables(grid)
    span, period = grid // RADIX, grid // WIDE
    chunks = rows // period
    dma = pltpu.SemaphoreType.DMA

    residual, shared, codes = pl.pallas_call(
        functools.partial(predict_kernel, group, beams, tiles_dev),
        out_shape=(
            jax.ShapeDtypeStruct((vis * 2, cells), f32),
            jax.ShapeDtypeStruct((group, vis, 2 * cells), bf16),
            jax.ShapeDtypeStruct((group, 8, lanes), jnp.int32),
        ),
        in_specs=[HBM, HBM, HBM, VMEM, VMEM, VMEM, VMEM, HBM, HBM, HBM, HBM],
        out_specs=(VMEM, VMEM, VMEM),
        scratch_shapes=[
            pltpu.VMEM((rows, strip), bf16),
            pltpu.VMEM((rows, halo), bf16),
            pltpu.VMEM((rows, halo), bf16),
            pltpu.VMEM((rows, grid), bf16),
            pltpu.VMEM((vis, cells, cells), bf16),
            pltpu.VMEM(real_table.shape, bf16),
            pltpu.VMEM(pair_table.shape, bf16),
            pltpu.VMEM(phase.shape, f32),
            pltpu.VMEM((chunks, *table.shape[1:]), bf16),
            pltpu.VMEM((8, lanes), jnp.int32),
            pltpu.SMEM((group, 8, lanes), jnp.int32),
            pltpu.VMEM((2, period, span), bf16),
            pltpu.VMEM((RADIX // 2 - 1, period, 2 * span), bf16),
            pltpu.VMEM((grid // 2 // RADIX, RADIX, period), f32),
            pltpu.VMEM((grid // 2 // RADIX, RADIX, period), f32),
            pltpu.VMEM((vis * RADIX, 2 * period), bf16),
            pltpu.VMEM((group * vis, 2 * cells), f32),
            pltpu.VMEM((group * vis, 2 * cells), bf16),
            pltpu.VMEM((group, vis, 2 * cells), bf16),
            pltpu.VMEM((vis, 2 * cells), bf16),
            pltpu.VMEM((vis * RADIX, cells), f32),
            pltpu.VMEM((vis * RADIX, cells), f32),
            dma((8,)),
            dma((2, chunks)), dma((2, chunks)),
            dma((group - 1,)), dma((group - 1,)),
            dma((group - 1,)), dma((group - 1,)),
            dma((group - 1,)), dma((group - 1,)),
        ],
        compiler_params=pltpu.CompilerParams(
            collective_id=0, has_side_effects=True, vmem_limit_bytes=60 * 1024 * 1024
        ),
        name="predict",
    )(
        sky_model, beam_pattern[0], kernels[0], observed.reshape(vis * 2, cells),
        tile_owner.reshape(1, vis), tile_local, vis_count,
        jnp.asarray(real_table), jnp.asarray(pair_table), jnp.asarray(phase), jnp.asarray(table),
    )

    blocks = 8
    dirty, residual = pl.pallas_call(
        functools.partial(dirty_kernel, vis),
        out_shape=(
            jax.ShapeDtypeStruct((tiles_dev * 2, cells), f32),
            jax.ShapeDtypeStruct((vis * 2, cells), f32),
        ),
        in_specs=[VMEM, VMEM, VMEM],
        out_specs=(HBM, VMEM),
        scratch_shapes=[pltpu.VMEM((blocks, tiles_dev * 2 // blocks, cells), f32), dma((blocks,))],
        name="dirty",
    )(codes, shared.reshape(group * vis, 2 * cells), residual)
    return (
        residual.reshape(1, vis, 2, cells),
        dirty.reshape(1, tiles_dev, 2, cells),
    )


def solution(mesh):
    placed = (
        P(("tile", "bl", "pol"), "beam"),
        P(("tile", "beam"), ("bl", "pol"), None),
        P(("tile", "beam"), ("bl", "pol"), None, None),
        P(("tile", "beam"), ("bl", "pol"), None, None),
        P(("tile", "beam"), ("bl", "pol"), None),
        P(("tile", "beam"), ("bl", "pol")),
        P(("tile", "beam"), ("bl", "pol")),
    )
    return jax.shard_map(
        on_device,
        mesh=mesh,
        in_specs=placed,
        out_specs=(
            P(("tile", "beam"), ("bl", "pol"), None, None),
            P(("tile", "beam"), ("bl", "pol"), None, None),
        ),
        check_vma=False,
    )
```
